32 devices in a mesh: seq: 16 (over z, x, core), res: 2 (over y).
Axes of the slice: x: 2, y: 2, z: 4, core: 2. Of those that a mesh axis runs over, the one named last changes fastest.
Arguments:
- alignment_rows: bfloat16 [1024, 16, 64], P('seq', 'res'), may hold values from -6 to 6
- pair_features: bfloat16 [16, 16, 128], P('res', 'seq'), may hold values from -6 to 6
- sequence_block_count: int32 [16], P('seq'), may hold values from 16 to 64
- cluster_member_count: int32 [1024], P('seq'), may hold values from 1 to 16
- residue_present_mask: int32 [16], replicated, may hold values 0 or 1
- attention_in_weight: bfloat16 [64, 256], replicated, may hold values from -0.75 to 0.75
- attention_out_weight: bfloat16 [64, 64], replicated, may hold values from -4 to 4
- pair_bias_weight: float32 [128, 8], replicated, may hold values from -48 to 48
- outer_factor_weight: bfloat16 [64, 64], replicated, may hold values from -0.75 to 0.75
- outer_output_weight: float32 [1024, 128], replicated, may hold values from -4 to 4
- outer_product_bias: float32 [128], replicated, may hold values from -3 to 3
Outputs:
- row_attention_update: bfloat16 [1024, 16, 64], P('seq', 'res')
- pair_update: bfloat16 [16, 16, 128], P('seq', 'res')
The draws below stay inside these ranges and needn't reach their ends.
All inputs are finite; a program needn't handle non-finite values.
Results may differ from the reference program's by a relative error of at most 0.0081.
Values may be sent and summed in bfloat16 or wider, within the bound.
A program may use at most 64 MiB of HBM per device.

```python
import math
import jax
import jax.numpy as jnp
from jax import lax

CHANNEL_COUNT = 64
CP = 128
CO = 32
HEADS = 8
HEAD_DIM = 8
SLOT_DEV = 64
RES_DEV = 8
SLOT_TOTAL = 1024
RESIDUE_TOTAL = 16
N_SEQ = 16
N_RES = 2


def draw_pair_bias_weight(key, part):
    values = jax.random.normal(key, (CP, HEADS), jnp.float32) * (2.0 / math.sqrt(CP))
    return jnp.clip(values, -48.0, 48.0)


def plant(values, key, low, top_value):
    index_at = [jax.random.randint(jax.random.fold_in(key, axis), (), 0, length) for axis, length in enumerate(values.shape)]
    widest = values.shape.index(max(values.shape))
    neighbour = index_at[:widest] + [(index_at[widest] + 1) % values.shape[widest]] + index_at[widest + 1:]
    return values.at[tuple(index_at)].set(low).at[tuple(neighbour)].set(top_value)


def level_of(key, shape, split, low, high):
    level = 1.0
    for position, blocks in split:
        steps = jax.random.uniform(jax.random.fold_in(jax.random.fold_in(key, 6), position), (blocks,), jnp.float32, low / len(split), high / len(split))
        level = level * jnp.repeat(jnp.exp(steps), shape[position] // blocks).reshape((-1,) + (1,) * (len(shape) - 1 - position))
    return level


def centred(rng, dims, scale, reach, split=(), kind=jnp.bfloat16):
    drawn = jax.random.normal(rng, dims, jnp.float32) * scale
    if len(split) > 0:
        drawn = level_of(rng, dims, split, -0.22, 0.18) * drawn
    return jnp.clip(drawn, min=-reach, max=reach).astype(kind)


def setup_inputs(seed: int = 0) -> dict:
    arg_keys = jax.random.split(jax.random.key(seed), 12)
    return {
        "alignment_rows": centred(arg_keys[0], (SLOT_TOTAL, RESIDUE_TOTAL, CHANNEL_COUNT), 1.0, 6.0, ((0, 16), (1, 2))),
        "pair_features": centred(arg_keys[1], (RESIDUE_TOTAL, RESIDUE_TOTAL, CP), 1.0, 6.0, ((0, 2), (1, 16))),
        "sequence_block_count": plant(jax.random.randint(arg_keys[2], (N_SEQ,), SLOT_DEV // 4, SLOT_DEV + 1), jax.random.fold_in(arg_keys[2], 1), SLOT_DEV // 4, SLOT_DEV).astype(jnp.int32),
        "cluster_member_count": plant(jax.random.randint(arg_keys[3], (SLOT_TOTAL,), 1, 17), jax.random.fold_in(arg_keys[3], 1), 1, 16).astype(jnp.int32),
        "residue_present_mask": plant((jax.random.randint(arg_keys[4], (RESIDUE_TOTAL,), 0, 8) < 7).astype(jnp.int32), jax.random.fold_in(arg_keys[4], 1), 0, 1),
        "attention_in_weight": centred(arg_keys[5], (CHANNEL_COUNT, 4 * CHANNEL_COUNT), CHANNEL_COUNT ** -0.5, 0.75),
        "attention_out_weight": centred(arg_keys[6], (CHANNEL_COUNT, CHANNEL_COUNT), 1.0, 4.0),
        "pair_bias_weight": draw_pair_bias_weight(jax.random.fold_in(arg_keys[11], 71), 0),
        "outer_factor_weight": centred(arg_keys[8], (CHANNEL_COUNT, 2 * CO), CHANNEL_COUNT ** -0.5, 0.75),
        "outer_output_weight": centred(arg_keys[9], (CO * CO, CP), 1.0, 4.0, (), jnp.float32),
        "outer_product_bias": centred(arg_keys[10], (CP,), 0.5, 3.0, (), jnp.float32),
    }


def apply_layer_norm(values):
    centre = lax.optimization_barrier(jnp.mean(values, axis=-1, keepdims=True))
    spread = lax.optimization_barrier(jnp.mean(jnp.square(values - centre), axis=-1, keepdims=True))
    return (values - centre) * lax.rsqrt(spread + 1e-05)

def attend_block(pieces, full_bias):
    query_rows, key_value_pairs, gate_activation = pieces
    slot_count, n_query, channel_width = query_rows.shape
    head_count = full_bias.shape[0]
    head_dim = channel_width // head_count
    n_keys = key_value_pairs.shape[1]
    query_heads = query_rows.astype(jnp.float32).reshape(slot_count, n_query, head_count, head_dim)
    key_heads = key_value_pairs[..., :channel_width].astype(jnp.float32).reshape(slot_count, n_keys, head_count, head_dim)
    value_heads = key_value_pairs[..., channel_width:].astype(jnp.float32).reshape(slot_count, n_keys, head_count, head_dim)
    scores = jnp.einsum('bihd,bjhd->bhij', query_heads, key_heads, precision=lax.Precision.HIGHEST) + full_bias[None]
    row_max = lax.optimization_barrier(jnp.max(scores, axis=-1, keepdims=True))
    expo = jnp.exp(scores - row_max)
    probs = (expo / lax.optimization_barrier(jnp.sum(expo, axis=-1, keepdims=True))).astype(jnp.bfloat16)
    context = jnp.einsum('bhij,bjhd->bihd', probs.astype(jnp.float32), value_heads, precision=lax.Precision.HIGHEST)
    return (gate_activation * context.reshape(slot_count, n_query, channel_width)).astype(jnp.bfloat16)

def reference(alignment_rows, pair_features, sequence_block_count, cluster_member_count, residue_present_mask, attention_in_weight, attention_out_weight, pair_bias_weight, outer_factor_weight, outer_output_weight, outer_product_bias):
    total_count = SLOT_DEV * N_SEQ
    block_length = RES_DEV * N_RES
    slot_ids = jnp.arange(total_count, dtype=jnp.int32)
    usable = (slot_ids % SLOT_DEV < sequence_block_count[slot_ids // SLOT_DEV]).astype(jnp.float32)
    seq_weight = cluster_member_count.astype(jnp.float32) * usable
    weight_sum = jnp.sum(seq_weight)
    key_mask = jnp.where(residue_present_mask == 1, 0.0, -1000000.0).astype(jnp.float32)
    pair_norm = apply_layer_norm(pair_features.astype(jnp.float32))
    pair_bias = jnp.einsum('ijp,ph->hij', pair_norm, pair_bias_weight, precision=lax.Precision.HIGHEST) + key_mask[None, None, :]
    normed_alignment = apply_layer_norm(alignment_rows.astype(jnp.float32)).astype(jnp.bfloat16)
    projected_rows = jnp.dot(normed_alignment.reshape(-1, CHANNEL_COUNT), attention_in_weight, preferred_element_type=jnp.float32).reshape(total_count, block_length, 4 * CHANNEL_COUNT)
    query_rows = (projected_rows[..., :CHANNEL_COUNT] * (1.0 / math.sqrt(HEAD_DIM))).astype(jnp.bfloat16)
    key_value_pairs = projected_rows[..., CHANNEL_COUNT:3 * CHANNEL_COUNT].astype(jnp.bfloat16)
    gate_activation = jax.nn.sigmoid(projected_rows[..., 3 * CHANNEL_COUNT:])
    gated = lax.map(lambda pieces: attend_block(pieces, pair_bias), (query_rows.reshape(N_SEQ, SLOT_DEV, block_length, CHANNEL_COUNT), key_value_pairs.reshape(N_SEQ, SLOT_DEV, block_length, 2 * CHANNEL_COUNT), gate_activation.reshape(N_SEQ, SLOT_DEV, block_length, CHANNEL_COUNT)))
    update = jnp.dot(gated.reshape(-1, CHANNEL_COUNT), attention_out_weight, preferred_element_type=jnp.float32).astype(jnp.bfloat16)
    row_attention_update = update.reshape(total_count, block_length, CHANNEL_COUNT) * usable.astype(jnp.bfloat16)[:, None, None]
    updated_alignment = alignment_rows.astype(jnp.float32) + row_attention_update.astype(jnp.float32)
    outer_input_norm = apply_layer_norm(updated_alignment).astype(jnp.bfloat16)
    factors = jnp.dot(outer_input_norm.reshape(-1, CHANNEL_COUNT), outer_factor_weight, preferred_element_type=jnp.float32).reshape(total_count, block_length, 2 * CO)
    res_keep = residue_present_mask.astype(jnp.float32)[None, :, None]
    left_proj = (factors[..., :CO] * res_keep).astype(jnp.bfloat16)
    right_proj = (factors[..., CO:] * res_keep * seq_weight[:, None, None]).astype(jnp.bfloat16)
    outer = lax.dot_general(left_proj.reshape(total_count, block_length * CO).astype(jnp.float32), right_proj.reshape(total_count, block_length * CO).astype(jnp.float32), (((0,), (0,)), ((), ())), precision=lax.Precision.HIGHEST)
    outer = outer.reshape(block_length, CO, block_length, CO)
    projected = jnp.einsum('icjd,cdp->ijp', outer, outer_output_weight.reshape(CO, CO, CP), precision=lax.Precision.HIGHEST)
    pair_update = (projected / weight_sum + outer_product_bias).astype(jnp.bfloat16)
    return (row_attention_update, pair_update)
```

```python
import functools
import math

import jax
import jax.numpy as jnp
from jax import lax
from jax.experimental import pallas as pl
from jax.experimental.pallas import tpu as pltpu
from jax.sharding import PartitionSpec as P

MESH = pl.DeviceIdType.MESH
F32 = jnp.float32
BF16 = jnp.bfloat16
LANES = 128


def dot(a, b, ca, cb, precision=None):
    return lax.dot_general(
        a, b, (((ca,), (cb,)), ((), ())), precision=precision, preferred_element_type=F32
    )


def norm_over(values, axis):
    centre = jnp.mean(values, axis=axis, keepdims=True)
    shifted = values - centre
    spread = jnp.mean(shifted * shifted, axis=axis, keepdims=True)
    return shifted * lax.rsqrt(spread + 1e-05)


def kernel(
    n_seq,
    n_res,
    slots,
    rl,
    heads,
    factor,
    count_ref,
    mask_ref,
    x_ref,
    pair_ref,
    members_ref,
    w_in_ref,
    w_out_ref,
    w_bias_ref,
    w_fac_ref,
    w_proj_hbm,
    bias_ref,
    update_ref,
    pair_out_ref,
    rows32,
    x_t,
    xn_buf,
    xn_recv,
    tile_buf,
    tile_recv,
    q_s,
    kv_s,
    roll_s,
    gate_s,
    bias_s,
    ctx_s,
    left_buf,
    left_recv,
    right_s,
    outer_s,
    w_raw,
    w_perm,
    part_buf,
    part_recv,
    w_sem,
    xn_send_sem,
    xn_recv_sem,
    tile_send_sem,
    tile_recv_sem,
    left_send_sem,
    left_recv_sem,
    part_send_sem,
    part_recv_sem,
):
    me_s = lax.axis_index("seq")
    me_r = lax.axis_index("res")
    width = x_ref.shape[2]
    hd = width // heads
    tiles = rl // 2
    n_keys = rl * n_res
    row_block = n_keys // n_seq
    key_block = pair_ref.shape[0] // rl

    def seq_peer(k):
        return lax.rem(me_s + k, n_seq)

    def res_peer(k):
        return lax.rem(me_r + k, n_res)

    barrier = pltpu.get_barrier_semaphore()

    @pl.loop(1, n_seq)
    def _(k):
        pl.semaphore_signal(barrier, inc=1, device_id=(seq_peer(k), me_r), device_id_type=MESH)

    for k in range(1, n_res):
        pl.semaphore_signal(barrier, inc=1, device_id=(me_s, res_peer(k)), device_id_type=MESH)

    w_copy = pltpu.make_async_copy(w_proj_hbm, w_raw, w_sem)
    w_copy.start()

    lane = lax.broadcasted_iota(jnp.int32, (1, LANES), 1)
    low = lane < slots
    count = count_ref[0]
    usable = (lax.rem(lane, slots) < count).astype(F32)
    members = members_ref[...].astype(F32)
    members = jnp.concatenate([members, members], axis=1)
    seq_weight = members * usable
    own_weight = jnp.sum(jnp.where(low, seq_weight, 0.0), axis=1, keepdims=True)

    pair_norm = norm_over(pair_ref[...].astype(F32), 1)
    pad = jnp.zeros((LANES - pair_norm.shape[0], pair_norm.shape[1]), F32)
    bias_t = dot(
        w_bias_ref[...], jnp.concatenate([pair_norm, pad], axis=0), 0, 1, lax.Precision.HIGHEST
    )
    tile_buf[...] = jnp.where(lane == LANES - 1, own_weight, bias_t)

    rows32[:, :width] = x_ref[...].astype(F32).reshape(slots * rl, width)
    eye = (
        lax.broadcasted_iota(jnp.int32, (width, width), 0)
        == lax.broadcasted_iota(jnp.int32, (width, width), 1)
    ).astype(F32).astype(BF16)
    for t in range(tiles):
        pair_rows = jnp.concatenate(
            [rows32[pl.ds(2 * t + e, slots, stride=rl), :][:, :width] for e in range(2)], axis=0
        ).astype(BF16)
        turned = dot(eye, pair_rows, 1, 1)
        x_t[t] = turned
        xn_buf[t] = norm_over(turned, 0).astype(BF16)

    pl.semaphore_wait(barrier, n_seq - 1 + n_res - 1)

    xn_copies = [
        pltpu.make_async_remote_copy(
            src_ref=xn_buf,
            dst_ref=xn_recv.at[k - 1],
            send_sem=xn_send_sem.at[k - 1],
            recv_sem=xn_recv_sem.at[k - 1],
            device_id=(me_s, res_peer(k)),
            device_id_type=MESH,
        )
        for k in range(1, n_res)
    ]
    for copy in xn_copies:
        copy.start()

    def tile_copy(k):
        return pltpu.make_async_remote_copy(
            src_ref=tile_buf,
            dst_ref=tile_recv.at[me_s],
            send_sem=tile_send_sem.at[k - 1],
            recv_sem=tile_recv_sem.at[k - 1],
            device_id=(seq_peer(k), me_r),
            device_id_type=MESH,
        )

    @pl.loop(1, n_seq)
    def _(k):
        tile_copy(k).start()

    tile_recv[me_s] = tile_buf[...]

    scale = 1.0 / math.sqrt(hd)

    def put_kv(block, t, kv):
        kv = kv.astype(BF16).astype(F32)
        kv_s[block, t] = kv
        roll_s[block, t] = pltpu.roll(kv, slots, 1)

    for t in range(tiles):
        proj = dot(w_in_ref[...], xn_buf[t], 0, 0)
        q_s[t] = (proj[:width] * scale).astype(BF16).astype(F32)
        put_kv(0, t, proj[width : 3 * width])
        gate_s[t] = jax.nn.sigmoid(proj[3 * width :])

    w_copy.wait()
    for d in range(factor):
        w_perm[d * factor : (d + 1) * factor] = w_raw[pl.ds(d, factor, stride=factor), :].astype(BF16)

    @pl.loop(1, n_seq)
    def _(k):
        tile_copy(k).wait()

    weight_sum = jnp.sum(tile_recv[...], axis=0)[:, LANES - 1 : LANES]

    def res_of(block):
        return lax.rem(me_r + n_res - block, n_res)

    for block in range(n_res):
        for u in range(tiles):
            keyed = []
            for e in range(2):
                j = res_of(block) * rl + 2 * u + e
                key_mask = jnp.where(mask_ref[j] == 1, 0.0, -1000000.0).astype(F32)
                tile = tile_recv[j // key_block] + key_mask
                j_in = j % key_block if key_block > 1 else 0
                if key_block > 1:
                    picks = [
                        jnp.sum(
                            jnp.where(lane == i * key_block + j_in, tile, 0.0), axis=1, keepdims=True
                        )
                        for i in range(rl)
                    ]
                else:
                    picks = [tile[:, i : i + 1] for i in range(rl)]
                keyed.append([jnp.broadcast_to(p, (heads, LANES)) for p in picks])
            for t in range(tiles):
                bias_s[t, 0, block, u] = jnp.where(low, keyed[0][2 * t], keyed[1][2 * t + 1])
                bias_s[t, 1, block, u] = jnp.where(low, keyed[1][2 * t], keyed[0][2 * t + 1])

    for block in range(1, n_res):
        xn_copies[block - 1].wait()
        for t in range(tiles):
            put_kv(block, t, dot(w_in_ref[:, width : 3 * width], xn_recv[block - 1, t], 0, 0))

    def heads_of(ref, base, d):
        return ref[pl.ds(base + d, heads, stride=hd), :]

    for t in range(tiles):
        queries = [q_s.at[t][pl.ds(d, heads, stride=hd), :] for d in range(hd)]
        scores = []
        for turn in range(2):
            source = roll_s if turn else kv_s
            for block in range(n_res):
                for u in range(tiles):
                    total = queries[0] * heads_of(source.at[block, u], 0, 0)
                    for d in range(1, hd):
                        total = total + queries[d] * heads_of(source.at[block, u], 0, d)
                    scores.append(total + bias_s[t, turn, block, u])
        top = functools.reduce(jnp.maximum, scores)
        expo = [jnp.exp(s - top) for s in scores]
        norm = 1.0 / functools.reduce(jnp.add, expo)
        probs = [(e * norm).astype(BF16).astype(F32) for e in expo]
        context = [None] * hd
        at = 0
        for turn in range(2):
            source = roll_s if turn else kv_s
            for block in range(n_res):
                for u in range(tiles):
                    for d in range(hd):
                        term = probs[at] * heads_of(source.at[block, u], width, d)
                        context[d] = term if context[d] is None else context[d] + term
                    at += 1
        for d in range(hd):
            ctx_s[t, pl.ds(d, heads, stride=hd), :] = context[d]

    gated_tiles = []
    keep_tiles = []
    for t in range(tiles):
        gated = (gate_s[t] * ctx_s[t]).astype(BF16)
        gated_tiles.append(gated)
        update = dot(w_out_ref[...], gated, 0, 0).astype(BF16).astype(F32) * usable
        outer_norm = norm_over(x_t[t] + update, 0).astype(BF16)
        factors = dot(w_fac_ref[...], outer_norm, 0, 0)
        keeps = [(mask_ref[me_r * rl + 2 * t + e]).astype(F32) for e in range(2)]
        keep = jnp.where(low, keeps[0], keeps[1])
        left_buf[t] = (factors[:factor] * keep).astype(BF16)
        right = factors[factor:] * keep * seq_weight
        turned = pltpu.roll(right, slots, 1)
        zero = jnp.zeros_like(right)
        right_s[0, pl.ds(2 * t, factor, stride=rl), :] = jnp.where(low, right, zero)
        right_s[0, pl.ds(2 * t + 1, factor, stride=rl), :] = jnp.where(low, turned, zero)
        right_s[1, pl.ds(2 * t, factor, stride=rl), :] = jnp.where(low, zero, turned)
        right_s[1, pl.ds(2 * t + 1, factor, stride=rl), :] = jnp.where(low, zero, right)

    left_copies = [
        pltpu.make_async_remote_copy(
            src_ref=left_buf,
            dst_ref=left_recv.at[k - 1],
            send_sem=left_send_sem.at[k - 1],
            recv_sem=left_recv_sem.at[k - 1],
            device_id=(me_s, res_peer(k)),
            device_id_type=MESH,
        )
        for k in range(1, n_res)
    ]
    for copy in left_copies:
        copy.start()

    right_all = right_s[...].reshape(2 * factor * rl, LANES).astype(BF16)
    groups = LANES // factor
    even = lax.rem(lane // factor, 2) == 0

    def project(block, left):
        products = dot(right_all, left.reshape(tiles * factor, LANES), 1, 1)
        for half in range(2):
            for g in range(factor // groups):
                base = (half * factor + g * groups) * rl
                a = [products[base + k * rl : base + (k + 1) * rl] for k in range(groups)]
                p0 = jnp.where(low, a[0], pltpu.roll(a[2], 64, 1))
                p2 = jnp.where(low, pltpu.roll(a[0], 64, 1), a[2])
                p1 = jnp.where(low, a[1], pltpu.roll(a[3], 64, 1))
                p3 = jnp.where(low, pltpu.roll(a[1], 64, 1), a[3])
                out = [
                    jnp.where(even, p0, pltpu.roll(p1, 32, 1)),
                    jnp.where(even, pltpu.roll(p0, 96, 1), p1),
                    jnp.where(even, p2, pltpu.roll(p3, 32, 1)),
                    jnp.where(even, pltpu.roll(p2, 96, 1), p3),
                ]
                for ip in range(groups):
                    i = 2 * ip + half
                    outer_s[i * rl : (i + 1) * rl, g * LANES : (g + 1) * LANES] = out[ip]
        part = dot(outer_s[...].astype(BF16), w_perm[...], 1, 0)
        part_buf[pl.ds(res_of(block) * rl, rl)] = part.reshape(rl, rl, part.shape[1])

    project(0, left_buf[...])

    row = lax.broadcasted_iota(jnp.int32, (slots, 1), 0)
    row_usable = (row < count).astype(F32)
    w_out_wide = jnp.concatenate([w_out_ref[...], w_out_ref[...]], axis=1)
    for t in range(tiles):
        plain = dot(gated_tiles[t], w_out_wide, 0, 0).astype(BF16).astype(F32)
        for e in range(2):
            rows32[pl.ds(2 * t + e, slots, stride=rl), :] = (
                plain[e * slots : (e + 1) * slots] * row_usable
            )
    update_ref[...] = rows32[:, :width].reshape(slots, rl, width).astype(BF16)

    for block in range(1, n_res):
        left_copies[block - 1].wait()
        project(block, left_recv[block - 1])

    def part_copy(k):
        owner = seq_peer(k)
        return pltpu.make_async_remote_copy(
            src_ref=part_buf.at[pl.ds(owner * row_block, row_block)],
            dst_ref=part_recv.at[k - 1],
            send_sem=part_send_sem.at[k - 1],
            recv_sem=part_recv_sem.at[k - 1],
            device_id=(owner, me_r),
            device_id_type=MESH,
        )

    @pl.loop(1, n_seq)
    def _(k):
        part_copy(k).start()

    @pl.loop(1, n_seq)
    def _(k):
        part_copy(k).wait()

    total = part_buf[pl.ds(me_s * row_block, row_block)] + jnp.sum(part_recv[...], axis=0)
    pair_out_ref[...] = (total / weight_sum[None] + bias_ref[...][None]).astype(BF16)


def solution(mesh):
    n_seq = mesh.shape["seq"]
    n_res = mesh.shape["res"]

    def local(
        alignment_rows,
        pair_features,
        sequence_block_count,
        cluster_member_count,
        residue_present_mask,
        attention_in_weight,
        attention_out_weight,
        pair_bias_weight,
        outer_factor_weight,
        outer_output_weight,
        outer_product_bias,
    ):
        slots, rl, width = alignment_rows.shape
        heads = pair_bias_weight.shape[1]
        factor = outer_factor_weight.shape[1] // 2
        pair_width = outer_output_weight.shape[1]
        key_block = pair_features.shape[1]
        row_block = rl * n_res // n_seq
        tiles = rl // 2
        assert 2 * slots == LANES and tiles * factor == LANES and 4 * factor == LANES
        assert pair_width == LANES and heads == 8 and rl == 8
        vmem = pl.BlockSpec(memory_space=pltpu.VMEM)
        smem = pl.BlockSpec(memory_space=pltpu.SMEM)
        dma = pltpu.SemaphoreType.DMA
        return pl.pallas_call(
            functools.partial(kernel, n_seq, n_res, slots, rl, heads, factor),
            out_shape=(
                jax.ShapeDtypeStruct((slots, rl, width), BF16),
                jax.ShapeDtypeStruct((row_block, rl, pair_width), BF16),
            ),
            in_specs=[smem, smem] + [vmem] * 7 + [pl.BlockSpec(memory_space=pl.ANY), vmem],
            out_specs=(vmem, vmem),
            scratch_shapes=[
                pltpu.VMEM((slots * rl, LANES), F32),
                pltpu.VMEM((tiles, width, LANES), F32),
                pltpu.VMEM((tiles, width, LANES), BF16),
                pltpu.VMEM((n_res - 1, tiles, width, LANES), BF16),
                pltpu.VMEM((heads, LANES), F32),
                pltpu.VMEM((n_seq, heads, LANES), F32),
                pltpu.VMEM((tiles, width, LANES), F32),
                pltpu.VMEM((n_res, tiles, 2 * width, LANES), F32),
                pltpu.VMEM((n_res, tiles, 2 * width, LANES), F32),
                pltpu.VMEM((tiles, width, LANES), F32),
                pltpu.VMEM((tiles, 2, n_res, tiles, heads, LANES), F32),
                pltpu.VMEM((tiles, width, LANES), F32),
                pltpu.VMEM((tiles, factor, LANES), BF16),
                pltpu.VMEM((n_res - 1, tiles, factor, LANES), BF16),
                pltpu.VMEM((2, factor * rl, LANES), F32),
                pltpu.VMEM((rl * rl, factor * factor), F32),
                pltpu.VMEM((factor * factor, pair_width), F32),
                pltpu.VMEM((factor * factor, pair_width), BF16),
                pltpu.VMEM((rl * n_res, rl, pair_width), F32),
                pltpu.VMEM((n_seq - 1, row_block, rl, pair_width), F32),
                dma,
                dma((n_res - 1,)),
                dma((n_res - 1,)),
                dma((n_seq - 1,)),
                dma((n_seq - 1,)),
                dma((n_res - 1,)),
                dma((n_res - 1,)),
                dma((n_seq - 1,)),
                dma((n_seq - 1,)),
            ],
            compiler_params=pltpu.CompilerParams(collective_id=0, has_side_effects=True),
        )(
            sequence_block_count,
            residue_present_mask,
            alignment_rows,
            pair_features.reshape(rl * key_block, pair_features.shape[2]),
            cluster_member_count.reshape(1, slots),
            attention_in_weight,
            attention_out_weight,
            pair_bias_weight,
            outer_factor_weight,
            outer_output_weight,
            outer_product_bias.reshape(1, pair_width),
        )

    return jax.shard_map(
        local,
        mesh=mesh,
        in_specs=(
            P("seq", "res", None),
            P("res", "seq", None),
            P("seq"),
            P("seq"),
            P(),
            P(),
            P(),
            P(),
            P(),
            P(),
            P(),
        ),
        out_specs=(P("seq", "res", None), P("seq", "res", None)),
        check_vma=False,
    )
```

```python
import functools
import math

import jax
import jax.numpy as jnp
from jax import lax
from jax.experimental import pallas as pl
from jax.experimental.pallas import tpu as pltpu
from jax.sharding import PartitionSpec as P

MESH = pl.DeviceIdType.MESH
F32 = jnp.float32
BF16 = jnp.bfloat16
LANES = 128


def dot(a, b, ca, cb, precision=None):
    return lax.dot_general(
        a, b, (((ca,), (cb,)), ((), ())), precision=precision, preferred_element_type=F32
    )


def norm_over(values, axis):
    centre = jnp.mean(values, axis=axis, keepdims=True)
    shifted = values - centre
    spread = jnp.mean(shifted * shifted, axis=axis, keepdims=True)
    return shifted * lax.rsqrt(spread + 1e-05)


def kernel(
    n_seq,
    n_res,
    slots,
    rl,
    heads,
    factor,
    count_ref,
    mask_ref,
    x_ref,
    pair_ref,
    members_ref,
    w_in_ref,
    w_out_ref,
    w_bias_ref,
    w_fac_ref,
    w_proj_hbm,
    bias_ref,
    update_ref,
    pair_out_ref,
    rows32,
    x_t,
    xn_buf,
    xn_recv,
    tile_buf,
    tile_recv,
    q_s,
    kv_s,
    roll_s,
    gate_s,
    bias_s,
    ctx_s,
    left_buf,
    left_recv,
    right_s,
    outer_s,
    w_raw,
    w_perm,
    part_buf,
    part_recv,
    w_sem,
    xn_send_sem,
    xn_recv_sem,
    tile_send_sem,
    tile_recv_sem,
    left_send_sem,
    left_recv_sem,
    part_send_sem,
    part_recv_sem,
):
    me_s = lax.axis_index("seq")
    me_r = lax.axis_index("res")
    width = x_ref.shape[2]
    hd = width // heads
    tiles = rl // 2
    n_keys = rl * n_res
    row_block = n_keys // n_seq
    key_block = pair_ref.shape[0] // rl

    def seq_peer(k):
        return lax.rem(me_s + k, n_seq)

    def res_peer(k):
        return lax.rem(me_r + k, n_res)

    barrier = pltpu.get_barrier_semaphore()

    @pl.loop(1, n_seq)
    def _(k):
        pl.semaphore_signal(barrier, inc=1, device_id=(seq_peer(k), me_r), device_id_type=MESH)

    for k in range(1, n_res):
        pl.semaphore_signal(barrier, inc=1, device_id=(me_s, res_peer(k)), device_id_type=MESH)

    w_copy = pltpu.make_async_copy(w_proj_hbm, w_raw, w_sem)
    w_copy.start()

    lane = lax.broadcasted_iota(jnp.int32, (1, LANES), 1)
    low = lane < slots
    count = count_ref[0]
    usable = (lax.rem(lane, slots) < count).astype(F32)
    members = members_ref[...].astype(F32)
    members = jnp.concatenate([members, members], axis=1)
    seq_weight = members * usable
    own_weight = jnp.sum(jnp.where(low, seq_weight, 0.0), axis=1, keepdims=True)

    pair_norm = norm_over(pair_ref[...].astype(F32), 1)
    pad = jnp.zeros((LANES - pair_norm.shape[0], pair_norm.shape[1]), F32)
    bias_t = dot(
        w_bias_ref[...], jnp.concatenate([pair_norm, pad], axis=0), 1, 1, lax.Precision.HIGHEST
    )
    tile_buf[...] = jnp.where(lane == LANES - 1, own_weight, bias_t)

    rows32[:, :width] = x_ref[...].astype(F32).reshape(slots * rl, width)
    eye = (
        lax.broadcasted_iota(jnp.int32, (width, width), 0)
        == lax.broadcasted_iota(jnp.int32, (width, width), 1)
    ).astype(F32).astype(BF16)
    for t in range(tiles):
        pair_rows = jnp.concatenate(
            [rows32[pl.ds(2 * t + e, slots, stride=rl), :][:, :width] for e in range(2)], axis=0
        ).astype(BF16)
        turned = dot(eye, pair_rows, 1, 1)
        x_t[t] = turned
        xn_buf[t] = norm_over(turned, 0).astype(BF16)

    pl.semaphore_wait(barrier, n_seq - 1 + n_res - 1)

    xn_copies = [
        pltpu.make_async_remote_copy(
            src_ref=xn_buf,
            dst_ref=xn_recv.at[k - 1],
            send_sem=xn_send_sem.at[k - 1],
            recv_sem=xn_recv_sem.at[k - 1],
            device_id=(me_s, res_peer(k)),
            device_id_type=MESH,
        )
        for k in range(1, n_res)
    ]
    for copy in xn_copies:
        copy.start()

    def tile_copy(k):
        return pltpu.make_async_remote_copy(
            src_ref=tile_buf,
            dst_ref=tile_recv.at[me_s],
            send_sem=tile_send_sem.at[k - 1],
            recv_sem=tile_recv_sem.at[k - 1],
            device_id=(seq_peer(k), me_r),
            device_id_type=MESH,
        )

    @pl.loop(1, n_seq)
    def _(k):
        tile_copy(k).start()

    tile_recv[me_s] = tile_buf[...]

    scale = 1.0 / math.sqrt(hd)

    def put_kv(block, t, kv):
        kv = kv.astype(BF16).astype(F32)
        kv_s[block, t] = kv
        roll_s[block, t] = pltpu.roll(kv, slots, 1)

    for t in range(tiles):
        proj = dot(w_in_ref[...], xn_buf[t], 0, 0)
        q_s[t] = (proj[:width] * scale).astype(BF16).astype(F32)
        put_kv(0, t, proj[width : 3 * width])
        gate_s[t] = jax.nn.sigmoid(proj[3 * width :])

    w_copy.wait()
    for d in range(factor):
        w_perm[d * factor : (d + 1) * factor] = w_raw[pl.ds(d, factor, stride=factor), :].astype(BF16)

    @pl.loop(1, n_seq)
    def _(k):
        tile_copy(k).wait()

    weight_sum = jnp.sum(tile_recv[...], axis=0)[:, LANES - 1 : LANES]

    def res_of(block):
        return lax.rem(me_r + n_res - block, n_res)

    for block in range(n_res):
        for u in range(tiles):
            keyed = []
            for e in range(2):
                j = res_of(block) * rl + 2 * u + e
                key_mask = jnp.where(mask_ref[j] == 1, 0.0, -1000000.0).astype(F32)
                tile = tile_recv[j // key_block] + key_mask
                j_in = j % key_block if key_block > 1 else 0
                if key_block > 1:
                    picks = [
                        jnp.sum(
                            jnp.where(lane == i * key_block + j_in, tile, 0.0), axis=1, keepdims=True
                        )
                        for i in range(rl)
                    ]
                else:
                    picks = [tile[:, i : i + 1] for i in range(rl)]
                keyed.append([jnp.broadcast_to(p, (heads, LANES)) for p in picks])
            for t in range(tiles):
                bias_s[t, 0, block, u] = jnp.where(low, keyed[0][2 * t], keyed[1][2 * t + 1])
                bias_s[t, 1, block, u] = jnp.where(low, keyed[1][2 * t], keyed[0][2 * t + 1])

    for block in range(1, n_res):
        xn_copies[block - 1].wait()
        for t in range(tiles):
            put_kv(block, t, dot(w_in_ref[:, width : 3 * width], xn_recv[block - 1, t], 0, 0))

    def heads_of(ref, base, d):
        return ref[pl.ds(base + d, heads, stride=hd), :]

    for t in range(tiles):
        queries = [q_s.at[t][pl.ds(d, heads, stride=hd), :] for d in range(hd)]
        scores = []
        for turn in range(2):
            source = roll_s if turn else kv_s
            for block in range(n_res):
                for u in range(tiles):
                    total = queries[0] * heads_of(source.at[block, u], 0, 0)
                    for d in range(1, hd):
                        total = total + queries[d] * heads_of(source.at[block, u], 0, d)
                    scores.append(total + bias_s[t, turn, block, u])
        top = functools.reduce(jnp.maximum, scores)
        expo = [jnp.exp(s - top) for s in scores]
        norm = 1.0 / functools.reduce(jnp.add, expo)
        probs = [(e * norm).astype(BF16).astype(F32) for e in expo]
        context = [None] * hd
        at = 0
        for turn in range(2):
            source = roll_s if turn else kv_s
            for block in range(n_res):
                for u in range(tiles):
                    for d in range(hd):
                        term = probs[at] * heads_of(source.at[block, u], width, d)
                        context[d] = term if context[d] is None else context[d] + term
                    at += 1
        for d in range(hd):
            ctx_s[t, pl.ds(d, heads, stride=hd), :] = context[d]

    gated_tiles = []
    keep_tiles = []
    for t in range(tiles):
        gated = (gate_s[t] * ctx_s[t]).astype(BF16)
        gated_tiles.append(gated)
        update = dot(w_out_ref[...], gated, 0, 0).astype(BF16).astype(F32) * usable
        outer_norm = norm_over(x_t[t] + update, 0).astype(BF16)
        factors = dot(w_fac_ref[...], outer_norm, 0, 0)
        keeps = [(mask_ref[me_r * rl + 2 * t + e]).astype(F32) for e in range(2)]
        keep = jnp.where(low, keeps[0], keeps[1])
        left_buf[t] = (factors[:factor] * keep).astype(BF16)
        right = factors[factor:] * keep * seq_weight
        turned = pltpu.roll(right, slots, 1)
        zero = jnp.zeros_like(right)
        right_s[0, pl.ds(2 * t, factor, stride=rl), :] = jnp.where(low, right, zero)
        right_s[0, pl.ds(2 * t + 1, factor, stride=rl), :] = jnp.where(low, turned, zero)
        right_s[1, pl.ds(2 * t, factor, stride=rl), :] = jnp.where(low, zero, turned)
        right_s[1, pl.ds(2 * t + 1, factor, stride=rl), :] = jnp.where(low, zero, right)

    left_copies = [
        pltpu.make_async_remote_copy(
            src_ref=left_buf,
            dst_ref=left_recv.at[k - 1],
            send_sem=left_send_sem.at[k - 1],
            recv_sem=left_recv_sem.at[k - 1],
            device_id=(me_s, res_peer(k)),
            device_id_type=MESH,
        )
        for k in range(1, n_res)
    ]
    for copy in left_copies:
        copy.start()

    right_all = right_s[...].reshape(2 * factor * rl, LANES).astype(BF16)
    groups = LANES // factor
    even = lax.rem(lane // factor, 2) == 0

    def project(block, left):
        products = dot(right_all, left.reshape(tiles * factor, LANES), 1, 1)
        for half in range(2):
            for g in range(factor // groups):
                base = (half * factor + g * groups) * rl
                a = [products[base + k * rl : base + (k + 1) * rl] for k in range(groups)]
                p0 = jnp.where(low, a[0], pltpu.roll(a[2], 64, 1))
                p2 = jnp.where(low, pltpu.roll(a[0], 64, 1), a[2])
                p1 = jnp.where(low, a[1], pltpu.roll(a[3], 64, 1))
                p3 = jnp.where(low, pltpu.roll(a[1], 64, 1), a[3])
                out = [
                    jnp.where(even, p0, pltpu.roll(p1, 32, 1)),
                    jnp.where(even, pltpu.roll(p0, 96, 1), p1),
                    jnp.where(even, p2, pltpu.roll(p3, 32, 1)),
                    jnp.where(even, pltpu.roll(p2, 96, 1), p3),
                ]
                for ip in range(groups):
                    i = 2 * ip + half
                    outer_s[i * rl : (i + 1) * rl, g * LANES : (g + 1) * LANES] = out[ip]
        part = dot(outer_s[...].astype(BF16), w_perm[...], 1, 0)
        part_buf[pl.ds(res_of(block) * rl, rl)] = part.reshape(rl, rl, part.shape[1])

    project(0, left_buf[...])

    row = lax.broadcasted_iota(jnp.int32, (slots, 1), 0)
    row_usable = (row < count).astype(F32)
    w_out_wide = jnp.concatenate([w_out_ref[...], w_out_ref[...]], axis=1)
    for t in range(tiles):
        plain = dot(gated_tiles[t], w_out_wide, 0, 0).astype(BF16).astype(F32)
        for e in range(2):
            rows32[pl.ds(2 * t + e, slots, stride=rl), :] = (
                plain[e * slots : (e + 1) * slots] * row_usable
            )
    update_ref[...] = rows32[:, :width].reshape(slots, rl, width).astype(BF16)

    for block in range(1, n_res):
        left_copies[block - 1].wait()
        project(block, left_recv[block - 1])

    def part_copy(k):
        owner = seq_peer(k)
        return pltpu.make_async_remote_copy(
            src_ref=part_buf.at[pl.ds(owner * row_block, row_block)],
            dst_ref=part_recv.at[k - 1],
            send_sem=part_send_sem.at[k - 1],
            recv_sem=part_recv_sem.at[k - 1],
            device_id=(owner, me_r),
            device_id_type=MESH,
        )

    @pl.loop(1, n_seq)
    def _(k):
        part_copy(k).start()

    @pl.loop(1, n_seq)
    def _(k):
        part_copy(k).wait()

    total = part_buf[pl.ds(me_s * row_block, row_block)] + jnp.sum(part_recv[...], axis=0)
    pair_out_ref[...] = (total / weight_sum[None] + bias_ref[...][None]).astype(BF16)


def solution(mesh):
    n_seq = mesh.shape["seq"]
    n_res = mesh.shape["res"]

    def local(
        alignment_rows,
        pair_features,
        sequence_block_count,
        cluster_member_count,
        residue_present_mask,
        attention_in_weight,
        attention_out_weight,
        pair_bias_weight,
        outer_factor_weight,
        outer_output_weight,
        outer_product_bias,
    ):
        slots, rl, width = alignment_rows.shape
        heads = pair_bias_weight.shape[1]
        factor = outer_factor_weight.shape[1] // 2
        pair_width = outer_output_weight.shape[1]
        key_block = pair_features.shape[1]
        row_block = rl * n_res // n_seq
        tiles = rl // 2
        assert 2 * slots == LANES and tiles * factor == LANES and 4 * factor == LANES
        assert pair_width == LANES and heads == 8 and rl == 8
        vmem = pl.BlockSpec(memory_space=pltpu.VMEM)
        smem = pl.BlockSpec(memory_space=pltpu.SMEM)
        dma = pltpu.SemaphoreType.DMA
        return pl.pallas_call(
            functools.partial(kernel, n_seq, n_res, slots, rl, heads, factor),
            out_shape=(
                jax.ShapeDtypeStruct((slots, rl, width), BF16),
                jax.ShapeDtypeStruct((row_block, rl, pair_width), BF16),
            ),
            in_specs=[smem, smem] + [vmem] * 7 + [pl.BlockSpec(memory_space=pl.ANY), vmem],
            out_specs=(vmem, vmem),
            scratch_shapes=[
                pltpu.VMEM((slots * rl, LANES), F32),
                pltpu.VMEM((tiles, width, LANES), F32),
                pltpu.VMEM((tiles, width, LANES), BF16),
                pltpu.VMEM((n_res - 1, tiles, width, LANES), BF16),
                pltpu.VMEM((heads, LANES), F32),
                pltpu.VMEM((n_seq, heads, LANES), F32),
                pltpu.VMEM((tiles, width, LANES), F32),
                pltpu.VMEM((n_res, tiles, 2 * width, LANES), F32),
                pltpu.VMEM((n_res, tiles, 2 * width, LANES), F32),
                pltpu.VMEM((tiles, width, LANES), F32),
                pltpu.VMEM((tiles, 2, n_res, tiles, heads, LANES), F32),
                pltpu.VMEM((tiles, width, LANES), F32),
                pltpu.VMEM((tiles, factor, LANES), BF16),
                pltpu.VMEM((n_res - 1, tiles, factor, LANES), BF16),
                pltpu.VMEM((2, factor * rl, LANES), F32),
                pltpu.VMEM((rl * rl, factor * factor), F32),
                pltpu.VMEM((factor * factor, pair_width), F32),
                pltpu.VMEM((factor * factor, pair_width), BF16),
                pltpu.VMEM((rl * n_res, rl, pair_width), F32),
                pltpu.VMEM((n_seq - 1, row_block, rl, pair_width), F32),
                dma,
                dma((n_res - 1,)),
                dma((n_res - 1,)),
                dma((n_seq - 1,)),
                dma((n_seq - 1,)),
                dma((n_res - 1,)),
                dma((n_res - 1,)),
                dma((n_seq - 1,)),
                dma((n_seq - 1,)),
            ],
            compiler_params=pltpu.CompilerParams(collective_id=0, has_side_effects=True),
        )(
            sequence_block_count,
            residue_present_mask,
            alignment_rows,
            pair_features.reshape(rl * key_block, pair_features.shape[2]),
            cluster_member_count.reshape(1, slots),
            attention_in_weight,
            attention_out_weight,
            pair_bias_weight.T,
            outer_factor_weight,
            outer_output_weight,
            outer_product_bias.reshape(1, pair_width),
        )

    return jax.shard_map(
        local,
        mesh=mesh,
        in_specs=(
            P("seq", "res", None),
            P("res", "seq", None),
            P("seq"),
            P("seq"),
            P(),
            P(),
            P(),
            P(),
            P(),
            P(),
            P(),
        ),
        out_specs=(P("seq", "res", None), P("seq", "res", None)),
        check_vma=False,
    )
```
